32 devices in a mesh: cell: 8 (over z, y), pool: 4 (over x, core).
Axes of the slice: x: 2, y: 2, z: 4, core: 2. Of those that a mesh axis runs over, the one named last changes fastest.
Arguments:
- fractions: bfloat16 [256, 8192], P(None, 'cell'), may hold values from 0 to 1, as said below
- order: int32 [8192], P('cell'), may hold values from 0 to 8191, as said below
- density: float32 [8, 16, 8192], P('pool', None, 'cell'), may hold values from 0.2 to 5
- area: float32 [16, 8192], P(None, 'cell'), may hold values from 0.05 to 3
- harvest: float32 [8], P('pool'), may hold values from 0.05 to 0.6
Outputs:
- new_density: float32 [8, 16, 8192], P('pool', None, 'cell')
- area_cum: float32 [16, 8192], P(None, 'cell')
- stock_mean: float32 [8, 16], P('pool')
- removed: float32 [16], replicated
The draws below stay inside these ranges and needn't reach their ends.
Inputs may be any that keep to these rules, and one draw needn't show every extreme that they name: A permutation of the cells; of the cells that one device holds in region order, every gridcell block of 1024 positions receives the same number. `fractions`: each column of a cell's matrix sums to one before rounding, with diagonal entries of 0.4 or more.
All inputs are finite; a program needn't handle non-finite values.
Results may differ from the reference program's by a relative error of at most 0.0003.
Values may be sent and summed in bfloat16 or wider, within the bound.
No kernel may reach another device: no remote copies, remote signals or barrier semaphores. Data moves between devices by JAX's collectives and lax.ppermute only.
A program may use at most 64 MiB of HBM per device.

```python
import math
import jax
import jax.numpy as jnp
from jax import lax

PFT = 16
POOLS = 8
CELL_DEV = 1024
CELLS = 8192


def draw_fractions(key, part):
    spread = jax.random.uniform(key, (16, 16, CELLS), jnp.float32, 0.0, 0.04)
    ident = jnp.eye(16, dtype=jnp.float32)[:, :, None]
    spread = spread * (1.0 - ident)
    keeping = 1.0 - jnp.sum(spread, axis=0, keepdims=True)
    whole = spread + ident * keeping
    return whole.reshape(256, CELLS).astype(jnp.bfloat16)


def draw_order(key, part):
    blocks = CELLS // CELL_DEV
    slots = CELL_DEV // blocks
    sources = jnp.arange(blocks)
    row_slot = jax.vmap(lambda s: jax.random.permutation(jax.random.fold_in(key, s), CELL_DEV))(sources)
    places = jax.vmap(lambda d: jax.random.permutation(jax.random.fold_in(key, blocks + d), CELL_DEV))(sources)
    target = row_slot // slots
    within = row_slot % slots
    position = target * CELL_DEV + places[target, sources[:, None] * slots + within]
    return position.reshape(CELLS).astype(jnp.int32)


def draw_area(key, part):
    blocks = CELLS // CELL_DEV
    base = jnp.exp(jax.random.uniform(key, (16, CELLS), jnp.float32, jnp.log(0.05), 0.0))
    rising = 1.0 + 2.0 * (jnp.arange(CELLS) // CELL_DEV).astype(jnp.float32) / max(blocks - 1, 1)
    return (base * rising[None]).astype(jnp.float32)


def level_of(own_key, dims, split, low, high):
    factor_of = 1.0
    for dim, shards_of in split:
        heights = jax.random.uniform(jax.random.fold_in(jax.random.fold_in(own_key, 6), dim), (shards_of,), jnp.float32, low / len(split), high / len(split))
        factor_of = factor_of * jnp.repeat(jnp.exp(heights), dims[dim] // shards_of).reshape((-1,) + (1,) * (len(dims) - 1 - dim))
    return factor_of


def setup_inputs(seed: int = 0) -> dict:
    splits = jax.random.split(jax.random.key(seed), 6)
    return {
        "fractions": draw_fractions(jax.random.fold_in(splits[5], 71), 0),
        "order": draw_order(jax.random.fold_in(splits[5], 71), 0),
        "density": jnp.clip(jnp.exp(math.log(5.0) - 3.218876 * jax.random.uniform(splits[2], (POOLS, PFT, CELLS), jnp.float32) ** level_of(splits[2], (POOLS, PFT, CELLS), ((0, 4), (2, 8)), -0.2, 0.2)), 0.2, 5.0),
        "area": draw_area(jax.random.fold_in(splits[5], 71), 0),
        "harvest": jnp.clip(jnp.exp(math.log(0.6) - 2.4849067 * jax.random.uniform(splits[4], (POOLS,), jnp.float32) ** level_of(splits[4], (POOLS,), ((0, 4),), -0.2, 0.2)), 0.05, 0.6),
    }


def transition(block_frac, density, area, harvest):
    matrix = block_frac.astype(jnp.float32).reshape(16, 16, -1)
    stock = area[None] * density
    total = jnp.einsum('ijc,pjc->pic', matrix, stock, precision=lax.Precision.HIGHEST)
    staying = block_frac.astype(jnp.float32)[::17]
    moved = total - staying[None] * stock
    new_stock = staying[None] * stock + (1.0 - harvest[:, None, None]) * moved
    new_area = jnp.einsum('ijc,jc->ic', matrix, area, precision=lax.Precision.HIGHEST)
    new_density = new_stock / new_area[None]
    area_cum = jnp.cumsum(new_area, axis=0) / jnp.sum(new_area, axis=0, keepdims=True)
    stock_sums = jnp.sum(new_stock, axis=2)
    removed_sums = jnp.sum(harvest[:, None, None] * moved, axis=(0, 2))
    return new_density, area_cum, stock_sums, removed_sums


def reference(fractions, order, density, area, harvest):
    block_frac = jnp.zeros_like(fractions).at[:, order].set(fractions)
    new_density, area_cum, stock_sums, removed_sums = transition(block_frac, density, area, harvest)
    return new_density, area_cum, stock_sums / CELLS, removed_sums / CELLS
```

```python
import functools

import jax
import jax.numpy as jnp
from jax import lax
from jax.experimental import pallas as pl
from jax.experimental.pallas import tpu as pltpu
from jax.sharding import PartitionSpec as P


LANES = 128
VMEM_LIMIT = 16 * 1024 * 1024
NT = (((1,), (1,)), ((), ()))
NN = (((1,), (0,)), ((), ()))
F32 = jnp.float32
BF16 = jnp.bfloat16


def iota(shape, dim):
    return lax.broadcasted_iota(jnp.int32, shape, dim)


def pack_kernel(targets_ref, frac_ref, order_ref, *out_refs, owned):
    count = len(out_refs)
    blocks = owned // LANES
    rows = -(-count // 8) * 8
    order = order_ref[...]
    dest = lax.shift_right_logical(order, owned.bit_length() - 1)
    local = order & (owned - 1)
    want = jnp.full((rows, LANES), -1, jnp.int32)
    for k in range(count):
        want = jnp.where(iota((rows, LANES), 0) == k, targets_ref[k], want)
    hits = [dest[:, b * LANES:(b + 1) * LANES] == want for b in range(blocks)]
    ones = jnp.concatenate([jnp.where(h, 1.0, 0.0) for h in hits], axis=0).astype(BF16)
    sums = jnp.where(iota((LANES, 2 * LANES), 0) < iota((LANES, 2 * LANES), 1), 1.0, 0.0).astype(BF16)
    prefix = lax.dot_general(ones, sums, NN, preferred_element_type=F32)
    before = jnp.zeros((rows, LANES), F32)
    slots = []
    for b in range(blocks):
        part = prefix[b * rows:(b + 1) * rows]
        slots.append(jnp.where(hits[b], part[:, :LANES] + before, -1.0).astype(jnp.int32))
        before = before + part[:, LANES:]
    slots = jnp.concatenate(slots, axis=1)
    high = lax.shift_right_logical(local, 7).astype(F32)
    low = (local & (LANES - 1)).astype(F32)
    which = iota((16, owned), 0)
    extra = jnp.where(which == 0, high, jnp.where(which == 1, low, 0.0)).astype(BF16)
    data = jnp.concatenate([frac_ref[...], extra], axis=0)
    width = out_refs[0].shape[1]
    for k in range(count):
        onehot = jnp.where(iota((width, owned), 0) == slots[k:k + 1], 1.0, 0.0).astype(BF16)
        out_refs[k][...] = lax.dot_general(data, onehot, NT, preferred_element_type=F32).astype(BF16)


def transition_kernel(harvest_ref, density_ref, area_ref, *refs, chunks):
    part_refs = refs[:chunks]
    density_out, cum_out, sums_out, block = refs[chunks:]
    pools, types, owned = density_ref.shape
    kinds = types * types
    blocks = owned // LANES
    parts = [ref[...] for ref in part_refs]
    held = owned // parts[0].shape[1]
    parts = parts[: held - 1] + [functools.reduce(jnp.add, parts[held - 1:])]
    data = jnp.concatenate(parts, axis=1)
    tail = data[kinds:].astype(F32)
    place = (tail[0:1] * LANES + tail[1:2]).astype(jnp.int32)
    onehot = jnp.where(iota((owned, owned), 0) == place, 1.0, 0.0).astype(BF16)
    placed = lax.dot_general(data[:kinds], onehot, NT, preferred_element_type=F32)
    for b in range(blocks):
        block[b * kinds:(b + 1) * kinds] = placed[:, b * LANES:(b + 1) * LANES]
    dest = iota((types, LANES), 0)
    sums = [jnp.zeros((types, LANES), F32) for _ in range(pools + 1)]
    for b in range(blocks):
        at = slice(b * LANES, (b + 1) * LANES)
        area = area_ref[:, at]
        stock = [area * density_ref[p, :, at] for p in range(pools)]
        sources = stock + [area]
        totals = [jnp.zeros((types, LANES), F32) for _ in sources]
        staying = jnp.zeros((types, LANES), F32)
        for j in range(types):
            column = block[pl.ds(b * kinds + j, types, stride=types), :]
            staying = jnp.where(dest == j, column, staying)
            totals = [t + column * s[j:j + 1] for t, s in zip(totals, sources)]
        new_area = totals[-1]
        inverse = 1.0 / new_area
        for p in range(pools):
            kept = staying * stock[p]
            moved = totals[p] - kept
            new_stock = kept + (1.0 - harvest_ref[p]) * moved
            density_out[p, :, at] = new_stock * inverse
            sums[p] = sums[p] + new_stock
            sums[pools] = sums[pools] + harvest_ref[p] * moved
        running = new_area
        step = 1
        while step < types:
            running = running + jnp.where(dest >= step, pltpu.roll(running, step, 0), 0.0)
            step *= 2
        cum_out[:, at] = running / running[types - 1:types]
    diagonal = dest == iota((types, LANES), 1)
    rows = []
    for s in sums:
        each = jnp.sum(s, axis=1, keepdims=True)
        rows.append(jnp.sum(jnp.where(diagonal, each, 0.0), axis=0, keepdims=True))
    rows.append(jnp.zeros((sums_out.shape[0] - len(rows), LANES), F32))
    sums_out[...] = jnp.concatenate(rows, axis=0)


def finish_kernel(sums_ref, removed_ref, mean_out, removed_out, *, scale):
    pools, types = mean_out.shape
    mean_out[...] = sums_ref[:pools, :types] * scale
    removed_out[...] = removed_ref[pools:pools + 1, :types] * scale


def fast_body(cells, pools_axis, fractions, order, density, area, harvest):
    kinds, owned = fractions.shape
    pools, types, _ = density.shape
    chunk = owned // cells
    cell = lax.axis_index("cell")
    core = lax.axis_index("pool") % 2
    hops = sorted(range(1, cells), key=lambda s: (bin(s).count("1"), s), reverse=True)
    even, odd = SPLIT.get(cells, (hops[0::2], hops[1::2]))
    targets = [cell] + [
        cell ^ jnp.where(core == 0, a, odd[k] if k < len(odd) else 0) for k, a in enumerate(even)
    ]
    vmem = pl.BlockSpec(memory_space=pltpu.VMEM)
    smem = pl.BlockSpec(memory_space=pltpu.SMEM)
    piece = jax.ShapeDtypeStruct((kinds + 16, chunk), BF16)
    packed = pl.pallas_call(
        functools.partial(pack_kernel, owned=owned),
        out_shape=[piece] * len(targets),
        in_specs=[smem, vmem, vmem],
        out_specs=[vmem] * len(targets),
        compiler_params=pltpu.CompilerParams(vmem_limit_bytes=VMEM_LIMIT),
        name="pack",
    )(jnp.stack(targets), fractions, order.reshape(1, owned))
    received = []
    for k, a in enumerate(even):
        b = odd[k] if k < len(odd) else None
        pairs = []
        for c in range(cells):
            for p in range(pools_axis):
                s = a if p % 2 == 0 else b
                if s is not None:
                    pairs.append((c * pools_axis + p, (c ^ s) * pools_axis + p))
        received.append(lax.ppermute(packed[1 + k], ("cell", "pool"), pairs))
    swap = [(p, p ^ 1) for p in range(pools_axis)]
    other = [lax.ppermute(r, "pool", swap) for r in received]
    parts = [packed[0]] + received[:-1] + other[:-1] + [received[-1], other[-1]]
    new_density, area_cum, sums = pl.pallas_call(
        functools.partial(transition_kernel, chunks=len(parts)),
        out_shape=[
            jax.ShapeDtypeStruct(density.shape, F32),
            jax.ShapeDtypeStruct(area.shape, F32),
            jax.ShapeDtypeStruct((8, LANES), F32),
        ],
        in_specs=[smem, vmem, vmem] + [vmem] * len(parts),
        out_specs=[vmem] * 3,
        scratch_shapes=[pltpu.VMEM((kinds * (owned // LANES), LANES), F32)],
        compiler_params=pltpu.CompilerParams(vmem_limit_bytes=VMEM_LIMIT),
        name="transition",
    )(harvest, density, area, *parts)
    step = 1
    while step < cells:
        sums = sums + lax.ppermute(sums, "cell", [(c, c ^ step) for c in range(cells)])
        step *= 2
    removed = sums
    step = 1
    while step < pools_axis:
        removed = removed + lax.ppermute(removed, "pool", [(p, p ^ step) for p in range(pools_axis)])
        step *= 2
    mean, removed = pl.pallas_call(
        functools.partial(finish_kernel, scale=1.0 / (cells * owned)),
        out_shape=[
            jax.ShapeDtypeStruct((pools, types), F32),
            jax.ShapeDtypeStruct((1, types), F32),
        ],
        in_specs=[vmem] * 2,
        out_specs=[vmem] * 2,
        compiler_params=pltpu.CompilerParams(vmem_limit_bytes=VMEM_LIMIT),
        name="finish",
    )(sums, removed)
    return new_density, area_cum, mean, removed.reshape(types)


SPLIT = {8: ((7, 3, 2, 1), (6, 5, 4))}


def place_columns(received, positions, owned):
    local = positions[0] - lax.axis_index("cell") * owned
    inverse = jnp.zeros((owned,), jnp.int32).at[local].set(jnp.arange(owned, dtype=jnp.int32))
    return jnp.take(received, inverse, axis=1)


def general_body(fractions, order, density, area, harvest):
    owned = fractions.shape[1]
    types = area.shape[0]
    grouping = jnp.argsort(order // owned, stable=True)
    positions = jnp.take(order, grouping).reshape(1, owned)
    outgoing = jnp.take(fractions, grouping, axis=1)
    received, got_pos = (
        lax.all_to_all(outgoing, "cell", split_axis=1, concat_axis=1, tiled=True),
        lax.all_to_all(positions, "cell", split_axis=1, concat_axis=1, tiled=True),
    )
    block_frac = place_columns(received, got_pos, owned)
    matrix = block_frac.astype(F32).reshape(types, types, owned)
    stock = area[None] * density
    total = jnp.einsum("ijc,pjc->pic", matrix, stock, precision=lax.Precision.HIGHEST)
    staying = block_frac.astype(F32)[:: types + 1]
    moved = total - staying[None] * stock
    new_stock = staying[None] * stock + (1.0 - harvest[:, None, None]) * moved
    new_area = jnp.einsum("ijc,jc->ic", matrix, area, precision=lax.Precision.HIGHEST)
    new_density = new_stock / new_area[None]
    area_cum = jnp.cumsum(new_area, axis=0) / jnp.sum(new_area, axis=0, keepdims=True)
    stock_local = jnp.sum(new_stock, axis=2)
    removed_local = jnp.sum(harvest[:, None, None] * moved, axis=(0, 2))
    stock_sums, removed_cells = lax.psum((stock_local, removed_local), "cell")
    removed_sums = lax.psum(removed_cells, "pool")
    count = lax.axis_size("cell") * owned
    return (new_density, area_cum, stock_sums / count, removed_sums / count)


def solution(mesh):
    cells, pools_axis = mesh.shape["cell"], mesh.shape["pool"]

    def body(fractions, order, density, area, harvest):
        kinds, owned = fractions.shape
        types = area.shape[0]
        fits = (
            cells in SPLIT
            and pools_axis & (pools_axis - 1) == 0
            and pools_axis > 1
            and owned & (owned - 1) == 0
            and owned % (cells * LANES) == 0
            and owned <= 256 * LANES
            and types % 8 == 0
            and types <= LANES
        )
        if fits:
            return fast_body(cells, pools_axis, fractions, order, density, area, harvest)
        return general_body(fractions, order, density, area, harvest)

    return jax.shard_map(
        body,
        mesh=mesh,
        in_specs=(P(None, "cell"), P("cell"), P("pool", None, "cell"), P(None, "cell"), P("pool")),
        out_specs=(P("pool", None, "cell"), P(None, "cell"), P("pool", None), P()),
        check_vma=False,
    )
```

```python
import functools

import jax
import jax.numpy as jnp
from jax import lax
from jax.experimental import pallas as pl
from jax.experimental.pallas import tpu as pltpu
from jax.sharding import PartitionSpec as P


LANES = 128
VMEM_LIMIT = 16 * 1024 * 1024
NT = (((1,), (1,)), ((), ()))
NN = (((1,), (0,)), ((), ()))
F32 = jnp.float32
BF16 = jnp.bfloat16


def iota(shape, dim):
    return lax.broadcasted_iota(jnp.int32, shape, dim)


def pack_kernel(*refs, even, odd):
    count = 1 + len(even)
    sources, (*out_refs, weighted_out), loaded, arrived = refs[:5], refs[5:6 + count], refs[6 + count:-1], refs[-1]
    order_vmem, frac, harvest, density, area = loaded
    copies = [
        pltpu.make_async_copy(source, target, arrived.at[n])
        for n, (source, target) in enumerate(zip(sources, loaded))
    ]
    for copy in copies:
        copy.start()
    _, owned = frac.shape
    blocks = owned // LANES
    rows = -(-count // 8) * 8
    cell = lax.axis_index("cell")
    core = lax.rem(lax.axis_index("pool"), 2)
    want = jnp.where(iota((rows, LANES), 0) == 0, cell, -1)
    for k, a in enumerate(even):
        target = cell ^ jnp.where(core == 0, a, odd[k] if k < len(odd) else 0)
        want = jnp.where(iota((rows, LANES), 0) == k + 1, target, want)
    sums = jnp.where(iota((LANES, 2 * LANES), 0) < iota((LANES, 2 * LANES), 1), 1.0, 0.0).astype(BF16)
    copies[0].wait()
    order = order_vmem[...]
    dest = lax.shift_right_logical(order, owned.bit_length() - 1)
    local = order & (owned - 1)
    hits = [dest[:, b * LANES:(b + 1) * LANES] == want for b in range(blocks)]
    ones = jnp.concatenate([jnp.where(h, 1.0, 0.0) for h in hits], axis=0).astype(BF16)
    prefix = lax.dot_general(ones, sums, NN, preferred_element_type=F32)
    before = jnp.zeros((rows, LANES), F32)
    slots = []
    for b in range(blocks):
        part = prefix[b * rows:(b + 1) * rows]
        slots.append(jnp.where(hits[b], part[:, :LANES] + before, -1.0))
        before = before + part[:, LANES:]
    slots = jnp.concatenate(slots, axis=1)
    width = out_refs[0].shape[1]
    onehot = jnp.concatenate([matches(slots[k:k + 1], width) for k in range(count)], axis=0)
    high = lax.shift_right_logical(local, 7).astype(F32)
    low = (local & (LANES - 1)).astype(F32)
    which = iota((16, owned), 0)
    extra = jnp.where(which == 0, high, jnp.where(which == 1, low, 0.0)).astype(BF16)
    for copy in copies[2:]:
        copy.wait()
    pools = density.shape[0]
    weighted_out[...] = area[...] * sum(harvest[:, p:p + 1] * density[p] for p in range(pools))
    copies[1].wait()
    data = jnp.concatenate([frac[...], extra], axis=0)
    packed = lax.dot_general(data, onehot, NT, preferred_element_type=F32).astype(BF16)
    for k in range(count):
        out_refs[k][...] = packed[:, k * width:(k + 1) * width]


def matches(row, height):
    steps = iota((height, row.shape[1]), 0).astype(F32).astype(BF16)
    one = jnp.ones(steps.shape, BF16)
    return jnp.where(steps == row.astype(BF16), one, jnp.zeros_like(one))


def placed(parts, kinds, owned):
    data = jnp.concatenate(parts, axis=1)
    tail = data[kinds:].astype(F32)
    high, low = tail[0:1], tail[1:2]
    onehot = jnp.concatenate(
        [matches(jnp.where(high == b, low, -1.0), LANES) for b in range(owned // LANES)], axis=0
    )
    return lax.dot_general(data[:kinds], onehot, NT, preferred_element_type=F32)


def place_kernel(*refs):
    kinds, owned = refs[-1].shape
    refs[-1][...] = placed([ref[...] for ref in refs[:-1]], kinds, owned).astype(BF16)


def transition_kernel(harvest_ref, density_ref, area_ref, weighted_a, weighted_b, early_ref, *refs, parts):
    stock_out, area_out, sums_out, block = refs[parts:]
    pools, types, owned = density_ref.shape
    kinds = types * types
    blocks = owned // LANES
    last = [ref[...] for ref in refs[:parts]]
    late = placed(last[:-2] + [last[-2] + last[-1]], kinds, owned) + early_ref[...].astype(F32)
    for b in range(blocks):
        block[b * kinds:(b + 1) * kinds] = late[:, b * LANES:(b + 1) * LANES]
    dest = iota((types, LANES), 0)
    sums = [jnp.zeros((types, LANES), F32) for _ in range(pools + 1)]
    for b in range(blocks):
        at = slice(b * LANES, (b + 1) * LANES)
        area = area_ref[:, at]
        stock = [area * density_ref[p, :, at] for p in range(pools)]
        sources = stock + [weighted_a[:, at] + weighted_b[:, at], area]
        totals = [jnp.zeros((types, LANES), F32) for _ in sources]
        staying = jnp.zeros((types, LANES), F32)
        for j in range(types):
            column = block[pl.ds(b * kinds + j, types, stride=types), :]
            staying = jnp.where(dest == j, column, staying)
            totals = [t + column * s[j:j + 1] for t, s in zip(totals, sources)]
        for p in range(pools):
            kept = staying * stock[p]
            new_stock = kept + (1.0 - harvest_ref[:, p:p + 1]) * (totals[p] - kept)
            stock_out[p, :, at] = new_stock
            sums[p] = sums[p] + new_stock
        sums[pools] = sums[pools] + (totals[pools] - staying * sources[pools])
        area_out[:, at] = totals[-1]
    diagonal = dest == iota((types, LANES), 1)
    rows = []
    for s in sums:
        each = jnp.sum(s, axis=1, keepdims=True)
        rows.append(jnp.sum(jnp.where(diagonal, each, 0.0), axis=0, keepdims=True))
    rows.append(jnp.zeros((sums_out.shape[0] - len(rows), LANES), F32))
    sums_out[...] = jnp.concatenate(rows, axis=0)


def density_kernel(stock_ref, area_ref, density_out, cum_out):
    pools, types, owned = stock_ref.shape
    running = area_ref[...]
    inverse = 1.0 / running
    for p in range(pools):
        density_out[p] = stock_ref[p] * inverse
    dest = iota((types, owned), 0)
    step = 1
    while step < types:
        running = running + jnp.where(dest >= step, pltpu.roll(running, step, 0), 0.0)
        step *= 2
    cum_out[...] = running / running[types - 1:types]


def finish_kernel(sums_a, sums_b, mean_out, removed_out, *, scale):
    pools, types = mean_out.shape
    sums = (sums_a[...] + sums_b[...]) * scale
    mean_out[...] = sums[:pools, :types]
    removed_out[...] = sums[pools:pools + 1, :types]


def call(kernel, out_shape, args, scratch=(), cost=None, space=pltpu.VMEM):
    vmem = pl.BlockSpec(memory_space=pltpu.VMEM)
    return pl.pallas_call(
        kernel,
        out_shape=out_shape,
        in_specs=[pl.BlockSpec(memory_space=space)] * len(args),
        out_specs=jax.tree.map(lambda _: vmem, out_shape),
        scratch_shapes=list(scratch),
        compiler_params=pltpu.CompilerParams(vmem_limit_bytes=VMEM_LIMIT),
        cost_estimate=cost,
    )(*args)


def array(*shape, dtype=F32):
    return jax.ShapeDtypeStruct(shape, dtype)


def fast_body(cells, pools_axis, fractions, order, density, area, harvest):
    kinds, owned = fractions.shape
    pools, types, _ = density.shape
    chunk = owned // cells
    even, odd = SPLIT[cells]
    count = 1 + len(even)
    harvest = harvest.reshape(1, pools)
    sources = (order.reshape(1, owned), fractions, harvest, density, area)
    *packed, weighted = call(
        functools.partial(pack_kernel, even=even, odd=odd),
        [array(kinds + 16, chunk, dtype=BF16)] * count + [array(types, owned)],
        [pltpu.with_memory_space_constraint(x, pltpu.HBM) for x in sources],
        scratch=[pltpu.VMEM(x.shape, x.dtype) for x in sources] + [pltpu.SemaphoreType.DMA((len(sources),))],
        space=pltpu.HBM,
    )
    received = []
    for k, a in enumerate(even):
        b = odd[k] if k < len(odd) else None
        pairs = []
        for c in range(cells):
            for p in range(pools_axis):
                s = a if p % 2 == 0 else b
                if s is not None:
                    pairs.append((c * pools_axis + p, (c ^ s) * pools_axis + p))
        received.append(lax.ppermute(packed[1 + k], ("cell", "pool"), pairs))
    other = []
    for r in received:
        other.append(swap(r, "pool", pools_axis, 1))
    step = 1
    while step < pools_axis // 2:
        weighted = weighted + swap(weighted, "pool", pools_axis, step)
        step *= 2
    weighted_far = swap(weighted, "pool", pools_axis, step)
    early = [packed[0]] + received[:-1] + other[:-2]
    placed_early = call(
        place_kernel,
        array(kinds, owned, dtype=BF16),
        early,
        cost=pl.CostEstimate(flops=2 * kinds * owned * owned, bytes_accessed=2 * kinds * owned, transcendentals=0),
    )
    late = [other[-2], received[-1], other[-1]]
    new_stock, new_area, sums = call(
        functools.partial(transition_kernel, parts=len(late)),
        [array(pools, types, owned), array(types, owned), array(8, LANES)],
        (harvest, density, area, weighted, weighted_far, placed_early, *late),
        scratch=[pltpu.VMEM((kinds * (owned // LANES), LANES), F32)],
    )
    new_density, area_cum = call(
        density_kernel, [array(pools, types, owned), array(types, owned)], (new_stock, new_area)
    )
    step = 1
    while step < cells // 2:
        sums = sums + swap(sums, "cell", cells, step)
        step *= 2
    last = swap(sums, "cell", cells, step)
    mean, removed = call(
        functools.partial(finish_kernel, scale=1.0 / (cells * owned)),
        [array(pools, types), array(1, types)],
        (sums, last),
    )
    return new_density, area_cum, mean, removed.reshape(types)


def swap(value, axis, size, step):
    return lax.ppermute(value, axis, [(n, n ^ step) for n in range(size)])


SPLIT = {8: ((6, 4, 2, 1), (7, 5, 3))}


def place_columns(received, positions, owned):
    local = positions[0] - lax.axis_index("cell") * owned
    inverse = jnp.zeros((owned,), jnp.int32).at[local].set(jnp.arange(owned, dtype=jnp.int32))
    return jnp.take(received, inverse, axis=1)


def general_body(fractions, order, density, area, harvest):
    owned = fractions.shape[1]
    types = area.shape[0]
    grouping = jnp.argsort(order // owned, stable=True)
    positions = jnp.take(order, grouping).reshape(1, owned)
    outgoing = jnp.take(fractions, grouping, axis=1)
    received, got_pos = (
        lax.all_to_all(outgoing, "cell", split_axis=1, concat_axis=1, tiled=True),
        lax.all_to_all(positions, "cell", split_axis=1, concat_axis=1, tiled=True),
    )
    block_frac = place_columns(received, got_pos, owned)
    matrix = block_frac.astype(F32).reshape(types, types, owned)
    stock = area[None] * density
    total = jnp.einsum("ijc,pjc->pic", matrix, stock, precision=lax.Precision.HIGHEST)
    staying = block_frac.astype(F32)[:: types + 1]
    moved = total - staying[None] * stock
    new_stock = staying[None] * stock + (1.0 - harvest[:, None, None]) * moved
    new_area = jnp.einsum("ijc,jc->ic", matrix, area, precision=lax.Precision.HIGHEST)
    new_density = new_stock / new_area[None]
    area_cum = jnp.cumsum(new_area, axis=0) / jnp.sum(new_area, axis=0, keepdims=True)
    stock_local = jnp.sum(new_stock, axis=2)
    removed_local = jnp.sum(harvest[:, None, None] * moved, axis=(0, 2))
    stock_sums, removed_cells = lax.psum((stock_local, removed_local), "cell")
    removed_sums = lax.psum(removed_cells, "pool")
    count = lax.axis_size("cell") * owned
    return (new_density, area_cum, stock_sums / count, removed_sums / count)


def solution(mesh):
    cells, pools_axis = mesh.shape["cell"], mesh.shape["pool"]

    def body(fractions, order, density, area, harvest):
        _, owned = fractions.shape
        types = area.shape[0]
        fits = (
            cells in SPLIT
            and pools_axis & (pools_axis - 1) == 0
            and pools_axis > 1
            and owned & (owned - 1) == 0
            and owned % (cells * LANES) == 0
            and owned <= 256 * LANES
            and types % 8 == 0
            and types <= LANES
        )
        if fits:
            return fast_body(cells, pools_axis, fractions, order, density, area, harvest)
        return general_body(fractions, order, density, area, harvest)

    return jax.shard_map(
        body,
        mesh=mesh,
        in_specs=(P(None, "cell"), P("cell"), P("pool", None, "cell"), P(None, "cell"), P("pool")),
        out_specs=(P("pool", None, "cell"), P(None, "cell"), P("pool", None), P()),
        check_vma=False,
    )
```

```python
import functools

import jax
import jax.numpy as jnp
from jax import lax
from jax.experimental import pallas as pl
from jax.experimental.pallas import tpu as pltpu
from jax.sharding import PartitionSpec as P


LANES = 128
VMEM_LIMIT = 16 * 1024 * 1024
NT = (((1,), (1,)), ((), ()))
NN = (((1,), (0,)), ((), ()))
F32 = jnp.float32
BF16 = jnp.bfloat16


def iota(shape, dim):
    return lax.broadcasted_iota(jnp.int32, shape, dim)


def pack_kernel(*refs, even, odd):
    count = 1 + len(even)
    sources, (*out_refs, weighted_out, split_out, harvest_out) = refs[:5], refs[5:8 + count]
    loaded, arrived = refs[8 + count:-1], refs[-1]
    order_vmem, frac, harvest, density, area = loaded
    copies = [
        pltpu.make_async_copy(source, target, arrived.at[n])
        for n, (source, target) in enumerate(zip(sources, loaded))
    ]
    for copy in copies:
        copy.start()
    _, owned = frac.shape
    blocks = owned // LANES
    rows = -(-count // 8) * 8
    cell = lax.axis_index("cell")
    core = lax.rem(lax.axis_index("pool"), 2)
    want = jnp.where(iota((rows, LANES), 0) == 0, cell, -1)
    for k, a in enumerate(even):
        target = cell ^ jnp.where(core == 0, a, odd[k])
        want = jnp.where(iota((rows, LANES), 0) == k + 1, target, want)
    sums = jnp.where(iota((LANES, 2 * LANES), 0) < iota((LANES, 2 * LANES), 1), 1.0, 0.0).astype(BF16)
    copies[0].wait()
    order = order_vmem[...]
    dest = lax.shift_right_logical(order, owned.bit_length() - 1)
    local = order & (owned - 1)
    hits = [dest[:, b * LANES:(b + 1) * LANES] == want for b in range(blocks)]
    ones = jnp.concatenate([jnp.where(h, 1.0, 0.0) for h in hits], axis=0).astype(BF16)
    prefix = lax.dot_general(ones, sums, NN, preferred_element_type=F32)
    before = jnp.zeros((rows, LANES), F32)
    slots = []
    for b in range(blocks):
        part = prefix[b * rows:(b + 1) * rows]
        slots.append(jnp.where(hits[b], part[:, :LANES] + before, -1.0))
        before = before + part[:, LANES:]
    slots = jnp.concatenate(slots, axis=1)
    width = out_refs[0].shape[1]
    onehot = jnp.concatenate([matches(slots[k:k + 1], width) for k in range(count)], axis=0)
    high = lax.shift_right_logical(local, 7).astype(F32)
    low = (local & (LANES - 1)).astype(F32)
    which = iota((16, owned), 0)
    extra = jnp.where(which == 0, high, jnp.where(which == 1, low, 0.0)).astype(BF16)
    for copy in copies[2:]:
        copy.wait()
    pools = density.shape[0]
    stock = [area[...] * density[p] for p in range(pools)]
    weighted_out[...] = sum(harvest[:, p:p + 1] * stock[p] for p in range(pools))
    harvest_out[...] = harvest[...]
    split_out[...] = in_parts(jnp.concatenate(stock, axis=0))
    copies[1].wait()
    data = jnp.concatenate([frac[...], extra], axis=0)
    packed = lax.dot_general(data, onehot, NT, preferred_element_type=F32).astype(BF16)
    for k in range(count):
        out_refs[k][...] = packed[:, k * width:(k + 1) * width]


def in_parts(values):
    parts = []
    for _ in range(3):
        parts.append(values.astype(BF16))
        values = values - parts[-1].astype(F32)
    return jnp.concatenate(parts, axis=0)


def matches(row, height):
    steps = iota((height, row.shape[1]), 0).astype(F32).astype(BF16)
    one = jnp.ones(steps.shape, BF16)
    return jnp.where(steps == row.astype(BF16), one, jnp.zeros_like(one))


def arrived_columns(refs, kinds, owned):
    parts = [ref[...] for ref in refs]
    data = jnp.concatenate(parts, axis=1)
    tail = data[kinds:].astype(F32)
    high, low = tail[0:1], tail[1:2]
    onehot = [matches(jnp.where(high == b, low, -1.0), LANES) for b in range(owned // LANES)]
    return data[:kinds], jnp.concatenate(onehot, axis=0)


def place_kernel(split_ref, *refs):
    *chunk_refs, placed_out, gram_out = refs
    data, onehot = arrived_columns(chunk_refs, *placed_out.shape)
    placed = lax.dot_general(data, onehot, NT, preferred_element_type=F32).astype(BF16)
    placed_out[...] = placed
    gram_out[...] = lax.dot_general(placed, split_ref[...], NT, preferred_element_type=F32)


def per_type(gram, types):
    gram = gram.reshape(types, types, gram.shape[1])
    own = iota(gram.shape, 1) == lax.rem(iota(gram.shape, 2), types)
    return jnp.sum(jnp.where(own, gram, 0.0), axis=1)


def sums_kernel(harvest_ref, weighted_a, weighted_b, split_ref, placed_ref, gram_ref, *refs):
    *chunk_refs, sums_out = refs
    kinds, owned = placed_ref.shape
    types = weighted_a.shape[0]
    pools = split_ref.shape[0] // (3 * types)
    data, onehot = arrived_columns(chunk_refs, kinds, owned)
    split = split_ref[...]
    weighted = in_parts(weighted_a[...] + weighted_b[...])
    late = lax.dot_general(jnp.concatenate([split, weighted], axis=0), onehot, NN, preferred_element_type=F32).astype(BF16)
    edge = split.shape[0]
    gram = gram_ref[...] + lax.dot_general(data, late[:edge], NT, preferred_element_type=F32)
    gram_weighted = lax.dot_general(placed_ref[...], weighted, NT, preferred_element_type=F32)
    gram_weighted = gram_weighted + lax.dot_general(data, late[edge:], NT, preferred_element_type=F32)
    rows = []
    diagonal = iota((types, LANES), 0) == iota((types, LANES), 1)
    by_lane = per_type(gram, types)
    lane = iota(by_lane.shape, 1)
    same = lax.rem(lane, types) == iota(by_lane.shape, 0)
    for p in range(pools):
        mine = lax.rem(lax.div(lane, types), pools) == p
        scale = jnp.where(same, 1.0, 1.0 - harvest_ref[:, p:p + 1])
        rows.append(jnp.sum(jnp.where(mine, by_lane * scale, 0.0), axis=1, keepdims=True))
    by_lane = per_type(gram_weighted, types)
    same = lax.rem(iota(by_lane.shape, 1), types) == iota(by_lane.shape, 0)
    rows.append(jnp.sum(jnp.where(same, 0.0, by_lane), axis=1, keepdims=True))
    rows = [jnp.sum(jnp.where(diagonal, r, 0.0), axis=0, keepdims=True) for r in rows]
    rows.append(jnp.zeros((sums_out.shape[0] - len(rows), LANES), F32))
    sums_out[...] = jnp.concatenate(rows, axis=0)


def density_kernel(harvest_ref, density_ref, area_ref, placed_ref, *refs):
    *chunk_refs, density_out, cum_out, block = refs
    pools, types, owned = density_ref.shape
    kinds = types * types
    blocks = owned // LANES
    data, onehot = arrived_columns(chunk_refs, kinds, owned)
    late = lax.dot_general(data, onehot, NT, preferred_element_type=F32) + placed_ref[...].astype(F32)
    for b in range(blocks):
        block[b * kinds:(b + 1) * kinds] = late[:, b * LANES:(b + 1) * LANES]
    dest = iota((types, LANES), 0)
    for b in range(blocks):
        at = slice(b * LANES, (b + 1) * LANES)
        area = area_ref[:, at]
        stock = [area * density_ref[p, :, at] for p in range(pools)]
        sources = stock + [area]
        totals = [jnp.zeros((types, LANES), F32) for _ in sources]
        staying = jnp.zeros((types, LANES), F32)
        for j in range(types):
            column = block[pl.ds(b * kinds + j, types, stride=types), :]
            staying = jnp.where(dest == j, column, staying)
            totals = [t + column * s[j:j + 1] for t, s in zip(totals, sources)]
        running = totals[-1]
        inverse = 1.0 / running
        for p in range(pools):
            kept = staying * stock[p]
            density_out[p, :, at] = (kept + (1.0 - harvest_ref[:, p:p + 1]) * (totals[p] - kept)) * inverse
        step = 1
        while step < types:
            running = running + jnp.where(dest >= step, pltpu.roll(running, step, 0), 0.0)
            step *= 2
        cum_out[:, at] = running / running[types - 1:types]


def finish_kernel(*refs, scale):
    *sums_refs, mean_out, removed_out = refs
    pools, types = mean_out.shape
    level = [ref[...] for ref in sums_refs]
    while len(level) > 1:
        level = [a + b for a, b in zip(level[0::2], level[1::2])]
    sums = level[0] * scale
    mean_out[...] = sums[:pools, :types]
    removed_out[...] = sums[pools:pools + 1, :types]


def call(kernel, out_shape, args, scratch=(), cost=None, space=pltpu.VMEM):
    vmem = pl.BlockSpec(memory_space=pltpu.VMEM)
    return pl.pallas_call(
        kernel,
        out_shape=out_shape,
        in_specs=[pl.BlockSpec(memory_space=space)] * len(args),
        out_specs=jax.tree.map(lambda _: vmem, out_shape),
        scratch_shapes=list(scratch),
        compiler_params=pltpu.CompilerParams(vmem_limit_bytes=VMEM_LIMIT),
        cost_estimate=cost,
    )(*args)


def array(*shape, dtype=F32):
    return jax.ShapeDtypeStruct(shape, dtype)


def fast_body(cells, pools_axis, fractions, order, density, area, harvest):
    kinds, owned = fractions.shape
    pools, types, _ = density.shape
    chunk = owned // cells
    even, odd = SPLIT[cells]
    count = 1 + len(even)
    harvest = harvest.reshape(1, pools)
    sources = (order.reshape(1, owned), fractions, harvest, density, area)
    *packed, weighted, split, harvest = call(
        functools.partial(pack_kernel, even=even, odd=odd),
        [array(kinds + 16, chunk, dtype=BF16)] * count
        + [array(types, owned), array(3 * pools * types, owned, dtype=BF16), array(1, pools)],
        [pltpu.with_memory_space_constraint(x, pltpu.HBM) for x in sources],
        scratch=[pltpu.VMEM(x.shape, x.dtype) for x in sources] + [pltpu.SemaphoreType.DMA((len(sources),))],
        space=pltpu.HBM,
    )
    received, other = [], []
    for k, hops in enumerate(zip(even, odd)):
        pairs = [
            (c * pools_axis + p, (c ^ hops[p % 2]) * pools_axis + p) for c in range(cells) for p in range(pools_axis)
        ]
        received.append(lax.ppermute(packed[1 + k], ("cell", "pool"), pairs))
        if hops[0] != hops[1]:
            other.append(swap(received[k], "pool", pools_axis, 1))
    step = 1
    while step < pools_axis // 2:
        weighted = weighted + swap(weighted, "pool", pools_axis, step)
        step *= 2
    weighted_far = swap(weighted, "pool", pools_axis, step)
    early = [packed[0]] + received[:-1] + other[:EARLY]
    placed, gram = call(place_kernel, [array(kinds, owned, dtype=BF16), array(kinds, split.shape[0])], (split, *early))
    late = other[EARLY:] + received[-1:]
    sums = call(sums_kernel, array(8, LANES), (harvest, weighted, weighted_far, split, placed, gram, *late))
    new_density, area_cum = call(
        density_kernel,
        [array(pools, types, owned), array(types, owned)],
        (harvest, density, area, placed, *late),
        scratch=[pltpu.VMEM((kinds * (owned // LANES), LANES), F32)],
    )
    step = cells // 2
    while step > 2:
        sums = sums + swap(sums, "cell", cells, step)
        step //= 2
    group = [sums]
    for n in range(1, min(4, cells)):
        group.append(swap(sums, "cell", cells, n))
    mean, removed = call(
        functools.partial(finish_kernel, scale=1.0 / (cells * owned)), [array(pools, types), array(1, types)], group
    )
    return new_density, area_cum, mean, removed.reshape(types)


def swap(value, axis, size, step):
    return lax.ppermute(value, axis, [(n, n ^ step) for n in range(size)])


SPLIT = {8: ((6, 2, 4, 1), (5, 7, 3, 1))}
EARLY = 1


def place_columns(received, positions, owned):
    local = positions[0] - lax.axis_index("cell") * owned
    inverse = jnp.zeros((owned,), jnp.int32).at[local].set(jnp.arange(owned, dtype=jnp.int32))
    return jnp.take(received, inverse, axis=1)


def general_body(fractions, order, density, area, harvest):
    owned = fractions.shape[1]
    types = area.shape[0]
    grouping = jnp.argsort(order // owned, stable=True)
    positions = jnp.take(order, grouping).reshape(1, owned)
    outgoing = jnp.take(fractions, grouping, axis=1)
    received, got_pos = (
        lax.all_to_all(outgoing, "cell", split_axis=1, concat_axis=1, tiled=True),
        lax.all_to_all(positions, "cell", split_axis=1, concat_axis=1, tiled=True),
    )
    block_frac = place_columns(received, got_pos, owned)
    matrix = block_frac.astype(F32).reshape(types, types, owned)
    stock = area[None] * density
    total = jnp.einsum("ijc,pjc->pic", matrix, stock, precision=lax.Precision.HIGHEST)
    staying = block_frac.astype(F32)[:: types + 1]
    moved = total - staying[None] * stock
    new_stock = staying[None] * stock + (1.0 - harvest[:, None, None]) * moved
    new_area = jnp.einsum("ijc,jc->ic", matrix, area, precision=lax.Precision.HIGHEST)
    new_density = new_stock / new_area[None]
    area_cum = jnp.cumsum(new_area, axis=0) / jnp.sum(new_area, axis=0, keepdims=True)
    stock_local = jnp.sum(new_stock, axis=2)
    removed_local = jnp.sum(harvest[:, None, None] * moved, axis=(0, 2))
    stock_sums, removed_cells = lax.psum((stock_local, removed_local), "cell")
    removed_sums = lax.psum(removed_cells, "pool")
    count = lax.axis_size("cell") * owned
    return (new_density, area_cum, stock_sums / count, removed_sums / count)


def solution(mesh):
    cells, pools_axis = mesh.shape["cell"], mesh.shape["pool"]

    def body(fractions, order, density, area, harvest):
        _, owned = fractions.shape
        types = area.shape[0]
        fits = (
            cells in SPLIT
            and pools_axis & (pools_axis - 1) == 0
            and pools_axis > 1
            and owned & (owned - 1) == 0
            and owned % (cells * LANES) == 0
            and owned <= 256 * LANES
            and types % 8 == 0
            and 3 * density.shape[0] * types <= LANES
        )
        if fits:
            return fast_body(cells, pools_axis, fractions, order, density, area, harvest)
        return general_body(fractions, order, density, area, harvest)

    return jax.shard_map(
        body,
        mesh=mesh,
        in_specs=(P(None, "cell"), P("cell"), P("pool", None, "cell"), P(None, "cell"), P("pool")),
        out_specs=(P("pool", None, "cell"), P(None, "cell"), P("pool", None), P()),
        check_vma=False,
    )
```

```python
import functools

import jax
import jax.numpy as jnp
from jax import lax
from jax.experimental import pallas as pl
from jax.experimental.pallas import tpu as pltpu
from jax.sharding import PartitionSpec as P


LANES = 128
VMEM_LIMIT = 16 * 1024 * 1024
NT = (((1,), (1,)), ((), ()))
NN = (((1,), (0,)), ((), ()))
F32 = jnp.float32
BF16 = jnp.bfloat16


def iota(shape, dim):
    return lax.broadcasted_iota(jnp.int32, shape, dim)


def pack_kernel(*refs, even, odd):
    count = 1 + len(even)
    sources, (*out_refs, weighted_out, split_out, harvest_out) = refs[:5], refs[5:8 + count]
    loaded, arrived = refs[8 + count:-1], refs[-1]
    order_vmem, frac, harvest, density, area = loaded
    copies = [
        pltpu.make_async_copy(source, target, arrived.at[n])
        for n, (source, target) in enumerate(zip(sources, loaded))
    ]
    for copy in copies:
        copy.start()
    _, owned = frac.shape
    blocks = owned // LANES
    rows = -(-count // 8) * 8
    cell = lax.axis_index("cell")
    core = lax.rem(lax.axis_index("pool"), 2)
    want = jnp.where(iota((rows, LANES), 0) == 0, cell, -1)
    for k, a in enumerate(even):
        target = cell ^ jnp.where(core == 0, a, odd[k])
        want = jnp.where(iota((rows, LANES), 0) == k + 1, target, want)
    sums = jnp.where(iota((LANES, 2 * LANES), 0) < iota((LANES, 2 * LANES), 1), 1.0, 0.0).astype(BF16)
    copies[0].wait()
    order = order_vmem[...]
    dest = lax.shift_right_logical(order, owned.bit_length() - 1)
    local = order & (owned - 1)
    hits = [dest[:, b * LANES:(b + 1) * LANES] == want for b in range(blocks)]
    ones = jnp.concatenate([jnp.where(h, 1.0, 0.0) for h in hits], axis=0).astype(BF16)
    prefix = lax.dot_general(ones, sums, NN, preferred_element_type=F32)
    before = jnp.zeros((rows, LANES), F32)
    slots = []
    for b in range(blocks):
        part = prefix[b * rows:(b + 1) * rows]
        slots.append(jnp.where(hits[b], part[:, :LANES] + before, -1.0))
        before = before + part[:, LANES:]
    slots = jnp.concatenate(slots, axis=1)
    width = out_refs[0].shape[1]
    onehot = jnp.concatenate([matches(slots[k:k + 1], width) for k in range(count)], axis=0)
    high = lax.shift_right_logical(local, 7).astype(F32)
    low = (local & (LANES - 1)).astype(F32)
    which = iota((8, owned), 0)
    extra = jnp.where(which == 0, high, jnp.where(which == 1, low, 0.0)).astype(BF16)
    for copy in copies[2:]:
        copy.wait()
    pools = density.shape[0]
    stock = [area[...] * density[p] for p in range(pools)]
    weighted_out[...] = sum(harvest[:, p:p + 1] * stock[p] for p in range(pools))
    harvest_out[...] = harvest[...]
    split_out[...] = in_parts(jnp.concatenate(stock, axis=0))
    copies[1].wait()
    data = jnp.concatenate([frac[...], extra], axis=0)
    packed = lax.dot_general(data, onehot, NT, preferred_element_type=F32).astype(BF16)
    for k in range(count):
        out_refs[k][...] = packed[:, k * width:(k + 1) * width]


def in_parts(values):
    parts = []
    for _ in range(3):
        parts.append(values.astype(BF16))
        values = values - parts[-1].astype(F32)
    return jnp.concatenate(parts, axis=0)


def matches(row, height):
    steps = iota((height, row.shape[1]), 0).astype(F32).astype(BF16)
    one = jnp.ones(steps.shape, BF16)
    return jnp.where(steps == row.astype(BF16), one, jnp.zeros_like(one))


def arrived_columns(refs, kinds, owned):
    parts = [ref[...] for ref in refs]
    data = jnp.concatenate(parts, axis=1)
    tail = data[kinds:].astype(F32)
    high, low = tail[0:1], tail[1:2]
    onehot = [matches(jnp.where(high == b, low, -1.0), LANES) for b in range(owned // LANES)]
    return data[:kinds], jnp.concatenate(onehot, axis=0)


def place_kernel(split_ref, *refs):
    *chunk_refs, placed_out, gram_out = refs
    data, onehot = arrived_columns(chunk_refs, *placed_out.shape)
    placed = lax.dot_general(data, onehot, NT, preferred_element_type=F32).astype(BF16)
    placed_out[...] = placed
    gram_out[...] = lax.dot_general(placed, split_ref[...], NT, preferred_element_type=F32)


def per_type(gram, types):
    gram = gram.reshape(types, types, gram.shape[1])
    own = iota(gram.shape, 1) == lax.rem(iota(gram.shape, 2), types)
    return jnp.sum(jnp.where(own, gram, 0.0), axis=1)


def sums_kernel(harvest_ref, weighted_a, weighted_b, split_ref, placed_ref, gram_ref, *refs):
    *chunk_refs, sums_out = refs
    kinds, owned = placed_ref.shape
    types = weighted_a.shape[0]
    pools = split_ref.shape[0] // (3 * types)
    data, onehot = arrived_columns(chunk_refs, kinds, owned)
    split = split_ref[...]
    weighted = in_parts(weighted_a[...] + weighted_b[...])
    late = lax.dot_general(jnp.concatenate([split, weighted], axis=0), onehot, NN, preferred_element_type=F32).astype(BF16)
    edge = split.shape[0]
    gram = gram_ref[...] + lax.dot_general(data, late[:edge], NT, preferred_element_type=F32)
    gram_weighted = lax.dot_general(placed_ref[...], weighted, NT, preferred_element_type=F32)
    gram_weighted = gram_weighted + lax.dot_general(data, late[edge:], NT, preferred_element_type=F32)
    rows = []
    diagonal = iota((types, LANES), 0) == iota((types, LANES), 1)
    by_lane = per_type(gram, types)
    lane = iota(by_lane.shape, 1)
    same = lax.rem(lane, types) == iota(by_lane.shape, 0)
    for p in range(pools):
        mine = lax.rem(lax.div(lane, types), pools) == p
        scale = jnp.where(same, 1.0, 1.0 - harvest_ref[:, p:p + 1])
        rows.append(jnp.sum(jnp.where(mine, by_lane * scale, 0.0), axis=1, keepdims=True))
    by_lane = per_type(gram_weighted, types)
    same = lax.rem(iota(by_lane.shape, 1), types) == iota(by_lane.shape, 0)
    rows.append(jnp.sum(jnp.where(same, 0.0, by_lane), axis=1, keepdims=True))
    rows = [jnp.sum(jnp.where(diagonal, r, 0.0), axis=0, keepdims=True) for r in rows]
    rows.append(jnp.zeros((sums_out.shape[0] - len(rows), LANES), F32))
    sums_out[...] = jnp.concatenate(rows, axis=0)


def density_kernel(harvest_ref, density_ref, area_ref, placed_ref, *refs):
    *chunk_refs, density_out, cum_out, block = refs
    pools, types, owned = density_ref.shape
    kinds = types * types
    blocks = owned // LANES
    data, onehot = arrived_columns(chunk_refs, kinds, owned)
    late = lax.dot_general(data, onehot, NT, preferred_element_type=F32) + placed_ref[...].astype(F32)
    for b in range(blocks):
        block[b * kinds:(b + 1) * kinds] = late[:, b * LANES:(b + 1) * LANES]
    dest = iota((types, LANES), 0)
    for b in range(blocks):
        at = slice(b * LANES, (b + 1) * LANES)
        area = area_ref[:, at]
        stock = [area * density_ref[p, :, at] for p in range(pools)]
        sources = stock + [area]
        totals = [jnp.zeros((types, LANES), F32) for _ in sources]
        staying = jnp.zeros((types, LANES), F32)
        for j in range(types):
            column = block[pl.ds(b * kinds + j, types, stride=types), :]
            staying = jnp.where(dest == j, column, staying)
            totals = [t + column * s[j:j + 1] for t, s in zip(totals, sources)]
        running = totals[-1]
        inverse = 1.0 / running
        for p in range(pools):
            kept = staying * stock[p]
            density_out[p, :, at] = (kept + (1.0 - harvest_ref[:, p:p + 1]) * (totals[p] - kept)) * inverse
        step = 1
        while step < types:
            running = running + jnp.where(dest >= step, pltpu.roll(running, step, 0), 0.0)
            step *= 2
        cum_out[:, at] = running / running[types - 1:types]


def finish_kernel(*refs, scale):
    *sums_refs, mean_out, removed_out = refs
    pools, types = mean_out.shape
    level = [ref[...] for ref in sums_refs]
    while len(level) > 1:
        level = [a + b for a, b in zip(level[0::2], level[1::2])]
    sums = level[0] * scale
    mean_out[...] = sums[:pools, :types]
    removed_out[...] = sums[pools:pools + 1, :types]


def call(kernel, out_shape, args, scratch=(), cost=None, space=pltpu.VMEM):
    vmem = pl.BlockSpec(memory_space=pltpu.VMEM)
    return pl.pallas_call(
        kernel,
        out_shape=out_shape,
        in_specs=[pl.BlockSpec(memory_space=space)] * len(args),
        out_specs=jax.tree.map(lambda _: vmem, out_shape),
        scratch_shapes=list(scratch),
        compiler_params=pltpu.CompilerParams(vmem_limit_bytes=VMEM_LIMIT),
        cost_estimate=cost,
    )(*args)


def array(*shape, dtype=F32):
    return jax.ShapeDtypeStruct(shape, dtype)


def fast_body(cells, pools_axis, fractions, order, density, area, harvest):
    kinds, owned = fractions.shape
    pools, types, _ = density.shape
    chunk = owned // cells
    even, odd = SPLIT[cells]
    count = 1 + len(even)
    harvest = harvest.reshape(1, pools)
    sources = (order.reshape(1, owned), fractions, harvest, density, area)
    *packed, weighted, split, harvest = call(
        functools.partial(pack_kernel, even=even, odd=odd),
        [array(kinds + 8, chunk, dtype=BF16)] * count
        + [array(types, owned), array(3 * pools * types, owned, dtype=BF16), array(1, pools)],
        [pltpu.with_memory_space_constraint(x, pltpu.HBM) for x in sources],
        scratch=[pltpu.VMEM(x.shape, x.dtype) for x in sources] + [pltpu.SemaphoreType.DMA((len(sources),))],
        space=pltpu.HBM,
    )
    received, other = [], []
    for k, hops in enumerate(zip(even, odd)):
        pairs = [
            (c * pools_axis + p, (c ^ hops[p % 2]) * pools_axis + p) for c in range(cells) for p in range(pools_axis)
        ]
        received.append(lax.ppermute(packed[1 + k], ("cell", "pool"), pairs))
        if hops[0] != hops[1]:
            other.append(swap(received[k], "pool", pools_axis, 1))
    step = 1
    while step < pools_axis // 2:
        weighted = weighted + swap(weighted, "pool", pools_axis, step)
        step *= 2
    weighted_far = swap(weighted, "pool", pools_axis, step)
    early = [packed[0]] + received[:-1] + other[:EARLY]
    placed, gram = call(place_kernel, [array(kinds, owned, dtype=BF16), array(kinds, split.shape[0])], (split, *early))
    late = other[EARLY:] + received[-1:]
    sums = call(sums_kernel, array(8, LANES), (harvest, weighted, weighted_far, split, placed, gram, *late))
    new_density, area_cum = call(
        density_kernel,
        [array(pools, types, owned), array(types, owned)],
        (harvest, density, area, placed, *late),
        scratch=[pltpu.VMEM((kinds * (owned // LANES), LANES), F32)],
    )
    step = cells // 2
    while step > 2:
        sums = sums + swap(sums, "cell", cells, step)
        step //= 2
    group = [sums]
    for n in range(1, min(4, cells)):
        group.append(swap(sums, "cell", cells, n))
    mean, removed = call(
        functools.partial(finish_kernel, scale=1.0 / (cells * owned)), [array(pools, types), array(1, types)], group
    )
    return new_density, area_cum, mean, removed.reshape(types)


def swap(value, axis, size, step):
    return lax.ppermute(value, axis, [(n, n ^ step) for n in range(size)])


SPLIT = {8: ((6, 4, 2, 1), (5, 7, 3, 1))}
EARLY = 1


def place_columns(received, positions, owned):
    local = positions[0] - lax.axis_index("cell") * owned
    inverse = jnp.zeros((owned,), jnp.int32).at[local].set(jnp.arange(owned, dtype=jnp.int32))
    return jnp.take(received, inverse, axis=1)


def general_body(fractions, order, density, area, harvest):
    owned = fractions.shape[1]
    types = area.shape[0]
    grouping = jnp.argsort(order // owned, stable=True)
    positions = jnp.take(order, grouping).reshape(1, owned)
    outgoing = jnp.take(fractions, grouping, axis=1)
    received, got_pos = (
        lax.all_to_all(outgoing, "cell", split_axis=1, concat_axis=1, tiled=True),
        lax.all_to_all(positions, "cell", split_axis=1, concat_axis=1, tiled=True),
    )
    block_frac = place_columns(received, got_pos, owned)
    matrix = block_frac.astype(F32).reshape(types, types, owned)
    stock = area[None] * density
    total = jnp.einsum("ijc,pjc->pic", matrix, stock, precision=lax.Precision.HIGHEST)
    staying = block_frac.astype(F32)[:: types + 1]
    moved = total - staying[None] * stock
    new_stock = staying[None] * stock + (1.0 - harvest[:, None, None]) * moved
    new_area = jnp.einsum("ijc,jc->ic", matrix, area, precision=lax.Precision.HIGHEST)
    new_density = new_stock / new_area[None]
    area_cum = jnp.cumsum(new_area, axis=0) / jnp.sum(new_area, axis=0, keepdims=True)
    stock_local = jnp.sum(new_stock, axis=2)
    removed_local = jnp.sum(harvest[:, None, None] * moved, axis=(0, 2))
    stock_sums, removed_cells = lax.psum((stock_local, removed_local), "cell")
    removed_sums = lax.psum(removed_cells, "pool")
    count = lax.axis_size("cell") * owned
    return (new_density, area_cum, stock_sums / count, removed_sums / count)


def solution(mesh):
    cells, pools_axis = mesh.shape["cell"], mesh.shape["pool"]

    def body(fractions, order, density, area, harvest):
        _, owned = fractions.shape
        types = area.shape[0]
        fits = (
            cells in SPLIT
            and pools_axis & (pools_axis - 1) == 0
            and pools_axis > 1
            and owned & (owned - 1) == 0
            and owned % (cells * LANES) == 0
            and owned <= 256 * LANES
            and types % 8 == 0
            and 3 * density.shape[0] * types <= LANES
        )
        if fits:
            return fast_body(cells, pools_axis, fractions, order, density, area, harvest)
        return general_body(fractions, order, density, area, harvest)

    return jax.shard_map(
        body,
        mesh=mesh,
        in_specs=(P(None, "cell"), P("cell"), P("pool", None, "cell"), P(None, "cell"), P("pool")),
        out_specs=(P("pool", None, "cell"), P(None, "cell"), P("pool", None), P()),
        check_vma=False,
    )
```
